32 devices in a mesh: col: 8 (over z, y), row: 4 (over x, core).
Axes of the slice: x: 2, y: 2, z: 4, core: 2. Of those that a mesh axis runs over, the one named last changes fastest.
Arguments:
- right_side: float32 [8192, 256], P(('row', 'col')), may hold values from -6 to 6
- prior_solution: bfloat16 [16384, 256], P('col'), may hold values from -6 to 6
- factor_codes: bfloat16 [8192, 16384], P('row', 'col'), may hold values from -0.046875 to 0.046875
- block_scale: float32 [4, 64], P('row', 'col'), may hold values from 0.3 to 3
- diag_inverse: bfloat16 [4, 2048, 2048], P('row', 'col'), may hold values from -0.125 to 0.125
- inner_factor: bfloat16 [4, 4, 2048, 2048], P('row', None, 'col'), may hold values from -0.125 to 0.125
Outputs:
- solved: float32 [8192, 256], P(('row', 'col'))
The draws below stay inside these ranges and needn't reach their ends.
All inputs are finite; a program needn't handle non-finite values.
Results may differ from the reference program's by a relative error of at most 0.0095.
Values may be sent and summed in bfloat16 or wider, within the bound.
No kernel may reach another device: no remote copies, remote signals or barrier semaphores. Data moves between devices by JAX's collectives and lax.ppermute only.
A program may use at most 64 MiB of HBM per device.

```python
import math
import jax
import jax.numpy as jnp
from jax import lax

PB = 2048
KB = 256
RHS = 256
PANELS = 4
K = 16384


def levels(rng, shape, cuts, smallest, high):
    gain = 1.0
    for position, blocks in cuts:
        steps = jax.random.uniform(jax.random.fold_in(jax.random.fold_in(rng, 6), position), (blocks,), jnp.float32, smallest / len(cuts), high / len(cuts))
        gain = gain * jnp.repeat(jnp.exp(steps), shape[position] // blocks).reshape((-1,) + (1,) * (len(shape) - 1 - position))
    return gain


def normal_values(stream_key, extent, deviation, reach, split=(), kind=jnp.bfloat16):
    drawn = deviation * jax.random.normal(stream_key, extent, jnp.float32)
    if split:
        drawn = drawn * levels(stream_key, extent, split, -0.22, 0.18)
    return jnp.clip(drawn, -reach, reach).astype(kind)


def setup_inputs(seed: int = 0) -> dict:
    streams_of = jax.random.split(jax.random.key(seed), 7)
    right_side = normal_values(streams_of[0], (PANELS * PB, RHS), 1.0, 6.0, ((0, 32),), jnp.float32)
    prior_solution = normal_values(streams_of[1], (K, RHS), 1.0, 6.0, ((0, 8),))
    factor_codes = normal_values(streams_of[2], (PANELS * PB, K), K ** -0.5, 0.046875, ((0, 4), (1, 8)))
    block_scale = jnp.clip(jnp.exp(math.log(3.0) - 2.3025851 * jax.random.uniform(streams_of[3], (PANELS, K // KB), jnp.float32) ** levels(streams_of[3], (PANELS, K // KB), ((0, 4), (1, 8)), -0.2, 0.2)), 0.3, 3.0)
    diag_inverse = normal_values(streams_of[4], (PANELS, PB, PB), PB ** -0.5, 0.125, ((0, 4), (1, 8)))
    inner_factor = normal_values(streams_of[5], (PANELS, PANELS, PB, PB), PB ** -0.5, 0.125, ((0, 4), (2, 8)))
    return dict(right_side=right_side, prior_solution=prior_solution, factor_codes=factor_codes, block_scale=block_scale, diag_inverse=diag_inverse, inner_factor=inner_factor)


def reference(right_side, prior_solution, factor_codes, block_scale, diag_inverse, inner_factor):
    panels = block_scale.shape[0]
    blocks_all = block_scale.shape[1]
    block_cols = factor_codes.shape[1] // blocks_all
    panel_rows = factor_codes.shape[0] // panels
    scale_rows = jnp.repeat(block_scale, panel_rows, axis=0)

    def add_block(summed, column_block):
        first = (column_block * block_cols).astype(jnp.int32)
        coded = lax.dynamic_slice_in_dim(factor_codes, first, block_cols, 1)
        earlier = lax.dynamic_slice_in_dim(prior_solution, first, block_cols, 0)
        scaling = lax.dynamic_slice_in_dim(scale_rows, column_block.astype(jnp.int32), 1, 1)
        return summed + scaling * jnp.dot(coded, earlier, preferred_element_type=jnp.float32), None

    initial = jnp.zeros((factor_codes.shape[0], prior_solution.shape[1]), jnp.float32)
    prior_term, _ = lax.scan(add_block, initial, jnp.arange(blocks_all, dtype=jnp.int32))
    rhs = right_side - prior_term
    outputs = []
    rounded_list = []
    for panel_index in range(panels):
        current = rhs[panel_index * panel_rows:(panel_index + 1) * panel_rows]
        for earlier_index in range(panel_index):
            current = current - jnp.dot(inner_factor[panel_index, earlier_index], rounded_list[earlier_index], preferred_element_type=jnp.float32)
        result = jnp.dot(diag_inverse[panel_index], current.astype(jnp.bfloat16), preferred_element_type=jnp.float32)
        outputs.append(result)
        rounded_list.append(result.astype(jnp.bfloat16))
    return jnp.concatenate(outputs, axis=0)
```

```python
import jax
import jax.numpy as jnp
from jax import lax
from jax.sharding import Mesh, PartitionSpec as P

AXES = ("cz", "cy", "rx", "rc")


def solution(mesh):
    cols, rows = mesh.shape["col"], mesh.shape["row"]
    sizes = (cols // 2, 2, rows // 2, 2)
    grid = Mesh(mesh.devices.reshape(sizes), AXES)
    count_z, _, count_x, _ = sizes
    bf16 = jnp.bfloat16

    def place(z, y, x, c):
        return ((z * 2 + y) * sizes[2] + x) * 2 + c

    def send(value, target, only=None):
        pairs = []
        for z in range(sizes[0]):
            for y in range(2):
                for x in range(sizes[2]):
                    for c in range(2):
                        if only is None or only(z, y, x, c):
                            pairs.append((place(z, y, x, c), place(*target(z, y, x, c))))
        return lax.ppermute(value, AXES, pairs)

    def over_y(z, y, x, c):
        return z, 1 - y, x, c

    def over_core(z, y, x, c):
        return z, y, x, 1 - c

    def odd_only(z, y, x, c):
        return c == 1

    def later_only(z, y, x, c):
        return x > 0

    def local(right_side, prior_solution, factor_codes, block_scale, diag_inverse, inner_factor):
        each, width = right_side.shape
        part = width // 4
        zed, why = lax.axis_index("cz"), lax.axis_index("cy")
        ex, core = lax.axis_index("rx"), lax.axis_index("rc")
        chunk = 2 * each
        panel = factor_codes.shape[0]

        def gather(piece):
            if count_z > 4:
                return jnp.moveaxis(lax.all_gather(piece, "cz", axis=0), 0, 1).reshape(part, panel)
            whole = jnp.zeros((part, panel), piece.dtype)
            got = [(zed, piece)]
            for step in range(1, count_z):
                moved = lax.ppermute(
                    piece, "cz", [(i, (i + step) % count_z) for i in range(count_z)]
                )
                got.append((lax.rem(zed + count_z - step, count_z), moved))
            for source, value in got:
                whole = lax.dynamic_update_slice(whole, value, (0, source * chunk))
            return whole

        def both_rows(inverse):
            beside = send(inverse, over_y)
            return inverse, beside

        def apply(pieces, vector):
            mine, beside = [
                lax.dot_general(
                    vector, piece, (((1,), (1,)), ((), ())), preferred_element_type=jnp.float32
                )
                for piece in pieces
            ]
            first = jnp.where(why == 0, mine, beside)
            second = jnp.where(why == 0, beside, mine)
            return jnp.concatenate([first, second], axis=1)

        def pick(even, odd):
            return jnp.where(core == 0, even, odd)

        inverse = diag_inverse[0]
        inverse_y = send(inverse, over_y)
        inverse_c = send(inverse, over_core)
        inverse_yc = send(inverse_y, over_core)
        inv_even = (pick(inverse, inverse_c), pick(inverse_y, inverse_yc))
        inv_odd = (pick(inverse_c, inverse), pick(inverse_yc, inverse_y))
        pair = lax.dynamic_index_in_dim(inner_factor[0], 2 * ex, 0, keepdims=False)
        pair_y = send(pair, over_y, odd_only)
        pair_c = send(pair, over_core, odd_only)
        pair_yc = send(pair_y, over_core, odd_only)
        link = (pick(pair_c, pair), pick(pair_yc, pair_y))
        before = 2 * (count_x - 1)
        past = inner_factor[0, :before]
        past_y = send(past, over_y, later_only)
        past_c = send(past, over_core, later_only)
        past_yc = send(past_y, over_core, later_only)
        past_even = (pick(past, past_c), pick(past_y, past_yc))
        past_odd = (pick(past_c, past), pick(past_yc, past_y))

        blocks = block_scale.shape[1]
        block_cols = prior_solution.shape[0] // blocks
        scaled = (
            prior_solution.astype(jnp.float32).reshape(blocks, block_cols, width)
            * block_scale[0][:, None, None]
        ).reshape(-1, width).astype(bf16)
        product = lax.dot_general(
            scaled, factor_codes, (((0,), (1,)), ((), ())), preferred_element_type=jnp.float32
        )
        spot = (zed * 2 + why) * each
        mine = lax.dynamic_slice(product, (0, spot), (width, each))
        partial = lax.dynamic_update_slice(-product, right_side.T - mine, (0, spot))
        parts = partial.astype(bf16).reshape(2, 2, part, count_z, chunk).transpose(3, 0, 1, 2, 4)
        parts = parts.reshape(count_z * 4, part, chunk)
        came = lax.all_to_all(parts, ("cz", "cy", "rc"), 0, 0)
        came = came.reshape(count_z * 2, 2, part, chunk).astype(jnp.float32).sum(0)
        rhs_even, rhs_odd = came[0], came[1]

        for turn in range(count_x):
            even = apply(inv_even, gather(rhs_even.astype(bf16)))
            even_all = gather(even.astype(bf16))
            current = rhs_odd - apply(link, even_all)
            odd = apply(inv_odd, gather(current.astype(bf16)))
            for later in range(turn + 1, count_x):

                def to_later(z, y, x, c):
                    return z, y, later, c

                def from_turn(z, y, x, c):
                    return x == turn

                seen_even = send(even_all, to_later, from_turn)
                seen_odd = gather(send(odd.astype(bf16), to_later, from_turn))
                for index, seen in ((2 * turn, seen_even), (2 * turn + 1, seen_odd)):
                    rhs_even = rhs_even - apply([p[index] for p in past_even], seen)
                    rhs_odd = rhs_odd - apply([p[index] for p in past_odd], seen)

        out = jnp.stack([even, odd]).reshape(2, part, 2, each).transpose(2, 0, 1, 3)
        out = lax.all_to_all(out.reshape(4, part, each), ("cy", "rc"), 0, 0)
        return out.reshape(width, each).T

    return jax.shard_map(
        local,
        mesh=grid,
        in_specs=(
            P(("rx", "rc", "cz", "cy"), None),
            P(("cz", "cy"), None),
            P(("rx", "rc"), ("cz", "cy")),
            P(("rx", "rc"), ("cz", "cy")),
            P(("rx", "rc"), ("cz", "cy"), None),
            P(("rx", "rc"), None, ("cz", "cy"), None),
        ),
        out_specs=P(("rx", "rc", "cz", "cy"), None),
        check_vma=False,
    )
```

```python
import jax
import jax.numpy as jnp
from jax import lax
from jax.experimental import pallas as pl
from jax.experimental.pallas import tpu as pltpu
from jax.sharding import Mesh, PartitionSpec as P

AXES = ("cz", "cy", "rx", "rc")


def solution(mesh):
    cols, rows = mesh.shape["col"], mesh.shape["row"]
    sizes = (cols // 2, 2, rows // 2, 2)
    grid = Mesh(mesh.devices.reshape(sizes), AXES)
    count_z, _, count_x, _ = sizes
    bf16 = jnp.bfloat16

    def place(z, y, x, c):
        return ((z * 2 + y) * sizes[2] + x) * 2 + c

    def send(value, target, only=None):
        pairs = []
        for z in range(sizes[0]):
            for y in range(2):
                for x in range(sizes[2]):
                    for c in range(2):
                        if only is None or only(z, y, x, c):
                            pairs.append((place(z, y, x, c), place(*target(z, y, x, c))))
        return lax.ppermute(value, AXES, pairs)

    def over_y(z, y, x, c):
        return z, 1 - y, x, c

    def over_core(z, y, x, c):
        return z, y, x, 1 - c

    def over_both(z, y, x, c):
        return z, 1 - y, x, 1 - c

    def picked(flag, why, vector, own, own_y, other, other_y, index):
        part, depth = vector.shape
        each = own.shape[1]

        def kernel(flags, vector_ref, own_ref, own_y_ref, other_ref, other_y_ref, out_ref, held, sems):
            def copies(first, second):
                return [
                    pltpu.make_async_copy(ref.at[index], held.at[slot], sems.at[slot])
                    for slot, ref in enumerate((first, second))
                ]

            @pl.when(flags[0] == 0)
            def _():
                for copy in copies(own_ref, own_y_ref):
                    copy.start()

            @pl.when(flags[0] != 0)
            def _():
                for copy in copies(other_ref, other_y_ref):
                    copy.start()

            results = []
            for slot, copy in enumerate(copies(own_ref, own_y_ref)):
                copy.wait()
                results.append(
                    lax.dot_general(
                        held[slot], vector_ref[...], (((1,), (1,)), ((), ())),
                        preferred_element_type=jnp.float32,
                    ).T
                )
            first = flags[1] == 0
            out_ref[:, :each] = jnp.where(first, results[0], results[1])
            out_ref[:, each:] = jnp.where(first, results[1], results[0])

        whole = pl.BlockSpec(memory_space=pltpu.VMEM)
        far = pl.BlockSpec(memory_space=pl.ANY)
        return pl.pallas_call(
            kernel,
            in_specs=[pl.BlockSpec(memory_space=pltpu.SMEM), whole, far, far, far, far],
            out_specs=whole,
            scratch_shapes=[
                pltpu.VMEM((2, each, depth), bf16),
                pltpu.SemaphoreType.DMA((2,)),
            ],
            out_shape=jax.ShapeDtypeStruct((part, 2 * each), jnp.float32),
            cost_estimate=pl.CostEstimate(
                flops=4 * part * depth * each,
                bytes_accessed=4 * each * depth,
                transcendentals=0,
            ),
            compiler_params=pltpu.CompilerParams(vmem_limit_bytes=8 * 1024 * 1024),
        )(jnp.stack([flag, why]).astype(jnp.int32), vector, own, own_y, other, other_y)

    def prior_parts(zed, why, right_side, prior_solution, factor_codes, block_scale):
        each, width = right_side.shape
        panel, depth = factor_codes.shape
        blocks = block_scale.shape[1]
        deep = depth // blocks
        chunk = 2 * each

        rows = chunk
        split = chunk // rows

        def kernel(place_ref, scale_ref, right_ref, prior_ref, codes_ref, out_ref, scaled, total):
            step = pl.program_id(0)

            @pl.when(step == 0)
            def _():
                for b in range(blocks):
                    part = prior_ref[b * deep : (b + 1) * deep, :].astype(jnp.float32)
                    scaled[b * deep : (b + 1) * deep, :] = (part * scale_ref[0, b]).astype(bf16)

            total[...] = -jnp.dot(
                codes_ref[...], scaled[...], preferred_element_type=jnp.float32
            )

            @pl.when(step == (place_ref[0] * 2 + place_ref[1]) // (rows // each))
            def _():
                first = 0 if rows == each else pl.multiple_of(place_ref[1] * each, each)
                total[pl.ds(first, each), :] += right_ref[...]

            out_ref[0] = total[...].T.astype(bf16)

        return pl.pallas_call(
            kernel,
            grid_spec=pltpu.PrefetchScalarGridSpec(
                num_scalar_prefetch=1,
                grid=(panel // rows,),
                in_specs=[
                    pl.BlockSpec(memory_space=pltpu.SMEM),
                    pl.BlockSpec((each, width), lambda i, p: (0, 0)),
                    pl.BlockSpec((depth, width), lambda i, p: (0, 0)),
                    pl.BlockSpec((rows, depth), lambda i, p: (i, 0)),
                ],
                out_specs=pl.BlockSpec((1, width, rows), lambda i, p: (i // split, 0, i % split)),
                scratch_shapes=[
                    pltpu.VMEM((depth, width), bf16),
                    pltpu.VMEM((rows, width), jnp.float32),
                ],
            ),
            out_shape=jax.ShapeDtypeStruct((panel // chunk, width, chunk), bf16),
            cost_estimate=pl.CostEstimate(
                flops=2 * panel * depth * width,
                bytes_accessed=2 * panel * depth + 4 * panel * width,
                transcendentals=0,
            ),
            compiler_params=pltpu.CompilerParams(vmem_limit_bytes=60 * 1024 * 1024),
        )(jnp.stack([zed, why]).astype(jnp.int32), block_scale, right_side, prior_solution, factor_codes)

    def over_y(z, y, x, c):
        return z, 1 - y, x, c

    def over_core(z, y, x, c):
        return z, y, x, 1 - c

    def over_both(z, y, x, c):
        return z, 1 - y, x, 1 - c

    def picked(flag, why, vector, own, own_y, other, other_y, index):
        part, depth = vector.shape
        each = own.shape[1]

        def kernel(flags, vector_ref, own_ref, own_y_ref, other_ref, other_y_ref, out_ref, held, sems):
            def copies(first, second):
                return [
                    pltpu.make_async_copy(ref.at[index], held.at[slot], sems.at[slot])
                    for slot, ref in enumerate((first, second))
                ]

            @pl.when(flags[0] == 0)
            def _():
                for copy in copies(own_ref, own_y_ref):
                    copy.start()

            @pl.when(flags[0] != 0)
            def _():
                for copy in copies(other_ref, other_y_ref):
                    copy.start()

            results = []
            for slot, copy in enumerate(copies(own_ref, own_y_ref)):
                copy.wait()
                results.append(
                    lax.dot_general(
                        held[slot], vector_ref[...], (((1,), (1,)), ((), ())),
                        preferred_element_type=jnp.float32,
                    ).T
                )
            first = flags[1] == 0
            out_ref[:, :each] = jnp.where(first, results[0], results[1])
            out_ref[:, each:] = jnp.where(first, results[1], results[0])

        whole = pl.BlockSpec(memory_space=pltpu.VMEM)
        far = pl.BlockSpec(memory_space=pl.ANY)
        return pl.pallas_call(
            kernel,
            in_specs=[pl.BlockSpec(memory_space=pltpu.SMEM), whole, far, far, far, far],
            out_specs=whole,
            scratch_shapes=[
                pltpu.VMEM((2, each, depth), bf16),
                pltpu.SemaphoreType.DMA((2,)),
            ],
            out_shape=jax.ShapeDtypeStruct((part, 2 * each), jnp.float32),
            cost_estimate=pl.CostEstimate(
                flops=4 * part * depth * each,
                bytes_accessed=4 * each * depth,
                transcendentals=0,
            ),
            compiler_params=pltpu.CompilerParams(vmem_limit_bytes=8 * 1024 * 1024),
        )(jnp.stack([flag, why]).astype(jnp.int32), vector, own, own_y, other, other_y)

    def prior_parts(zed, why, right_side, prior_solution, factor_codes, block_scale):
        each, width = right_side.shape
        panel, depth = factor_codes.shape
        blocks = block_scale.shape[1]
        deep = depth // blocks
        chunk = 2 * each

        def kernel(place_ref, scale_ref, right_ref, prior_ref, codes_ref, out_ref, scaled, total):
            step = pl.program_id(0)

            @pl.when(step == 0)
            def _():
                for b in range(blocks):
                    part = prior_ref[b * deep : (b + 1) * deep, :].astype(jnp.float32)
                    scaled[b * deep : (b + 1) * deep, :] = (part * scale_ref[0, b]).astype(bf16)

            total[...] = -jnp.dot(
                codes_ref[...], scaled[...], preferred_element_type=jnp.float32
            )

            @pl.when(step == place_ref[0])
            def _():
                rows = pl.ds(pl.multiple_of(place_ref[1] * each, each), each)
                total[rows, :] += right_ref[...]

            out_ref[0] = total[...].T.astype(bf16)

        return pl.pallas_call(
            kernel,
            grid_spec=pltpu.PrefetchScalarGridSpec(
                num_scalar_prefetch=1,
                grid=(panel // chunk,),
                in_specs=[
                    pl.BlockSpec(memory_space=pltpu.SMEM),
                    pl.BlockSpec((each, width), lambda i, p: (0, 0)),
                    pl.BlockSpec((depth, width), lambda i, p: (0, 0)),
                    pl.BlockSpec((chunk, depth), lambda i, p: (i, 0)),
                ],
                out_specs=pl.BlockSpec((1, width, chunk), lambda i, p: (i, 0, 0)),
                scratch_shapes=[
                    pltpu.VMEM((depth, width), bf16),
                    pltpu.VMEM((chunk, width), jnp.float32),
                ],
            ),
            out_shape=jax.ShapeDtypeStruct((panel // chunk, width, chunk), bf16),
            cost_estimate=pl.CostEstimate(
                flops=2 * panel * depth * width,
                bytes_accessed=2 * panel * depth + 4 * panel * width,
                transcendentals=0,
            ),
            compiler_params=pltpu.CompilerParams(vmem_limit_bytes=60 * 1024 * 1024),
        )(jnp.stack([zed, why]).astype(jnp.int32), block_scale, right_side, prior_solution, factor_codes)

    def local(right_side, prior_solution, factor_codes, block_scale, diag_inverse, inner_factor):
        each, width = right_side.shape
        part = width // 4
        zed, why = lax.axis_index("cz"), lax.axis_index("cy")
        ex, core = lax.axis_index("rx"), lax.axis_index("rc")
        chunk = 2 * each
        panel = factor_codes.shape[0]

        def gather(piece):
            if count_z > 4:
                return jnp.moveaxis(lax.all_gather(piece, "cz", axis=0), 0, 1).reshape(part, panel)
            whole = jnp.zeros((part, panel), piece.dtype)
            got = [(zed, piece)]
            for step in range(1, count_z):

                def along(z, y, x, c):
                    return (z + step) % count_z, y, x, c

                moved = send(piece, along)
                got.append((lax.rem(zed + count_z - step, count_z), moved))
            for source, value in got:
                whole = lax.dynamic_update_slice(whole, value, (0, source * chunk))
            return whole

        def apply(pieces, vector):
            mine, beside = [
                lax.dot_general(
                    vector, piece, (((1,), (1,)), ((), ())), preferred_element_type=jnp.float32
                )
                for piece in pieces
            ]
            first = jnp.where(why == 0, mine, beside)
            second = jnp.where(why == 0, beside, mine)
            return jnp.concatenate([first, second], axis=1)

        def pick(even, odd):
            return lax.optimization_barrier(jnp.where(core == 0, even, odd))

        before = 2 * (count_x - 1)
        inverse = diag_inverse[0]
        turns = range(count_x)

        def odd_at(turn):
            return lambda z, y, x, c: x == turn and c == 1

        inverse_y = send(inverse, over_y)
        past = inner_factor[0, :before]
        past_y = send(past, over_y, lambda z, y, x, c: x > 0)
        pair = lax.dynamic_index_in_dim(inner_factor[0], 2 * ex, 0, keepdims=False)
        inverse_c = send(inverse, over_core)
        pair_c = send(pair, over_core)
        past_c = send(past, over_core)
        inverse_yc = send(inverse_y, over_core)
        past_yc = send(past_y, over_core)
        pair_y, pair_yc = {}, {}
        for turn in turns:
            pair_y[turn] = send(pair, over_y, odd_at(turn))
            pair_yc[turn] = send(pair_y[turn], over_core)
        inv_even = (pick(inverse, inverse_c), pick(inverse_y, inverse_yc))
        inv_odd = (pick(inverse_c, inverse), pick(inverse_yc, inverse_y))
        near_link = pick(pair_c, pair)
        link = {}
        for turn in turns:
            link[turn] = (near_link, pick(pair_yc[turn], pair_y[turn]))

        parts = prior_parts(zed, why, right_side, prior_solution, factor_codes, block_scale)
        parts = parts.reshape(count_z * 4, part, chunk)
        came = lax.all_to_all(parts, ("cz", "cy", "rc"), 0, 0)
        came = came.reshape(count_z * 2, 2, part, chunk).astype(jnp.float32).sum(0)
        rhs_even, rhs_odd = came[0], came[1]

        for turn in range(count_x):
            vector = gather(rhs_even.astype(bf16))
            even = apply(inv_even, vector)
            even_all = gather(even.astype(bf16))
            current = rhs_odd - apply(link[turn], even_all)
            vector = gather(current.astype(bf16))
            odd = apply(inv_odd, vector)
            kept = odd if turn == 0 else jnp.where(ex == turn, odd, kept)
            for later in range(turn + 1, count_x):

                def exchange(z, y, x, c):
                    return z, y, later if x == turn else turn if x == later else x, c

                seen_even = send(even_all, exchange)
                moved = send(odd.astype(bf16), exchange)
                seen_odd = gather(moved)
                here = ex == later
                for index, seen in ((2 * turn, seen_even), (2 * turn + 1, seen_odd)):
                    add = picked(core, why, seen, past, past_y, past_c, past_yc, index)
                    rhs_even = rhs_even - jnp.where(here, add, 0.0)
                    add = picked(1 - core, why, seen, past, past_y, past_c, past_yc, index)
                    rhs_odd = rhs_odd - jnp.where(here, add, 0.0)

        near = [jnp.where(why == 0, v[:, :each], v[:, each:]) for v in (even, kept)]
        far = [jnp.where(why == 0, v[:, each:], v[:, :each]) for v in (even, kept)]
        mine = jnp.where(core == 0, near[0], near[1])
        from_c = send(jnp.where(core == 0, near[1], near[0]), over_core)
        from_y = send(jnp.where(core == 0, far[0], far[1]), over_y)
        from_yc = send(jnp.where(core == 0, far[1], far[0]), over_both)
        by_y = [
            (jnp.where(core == 0, v, w), jnp.where(core == 0, w, v))
            for v, w in ((mine, from_c), (from_y, from_yc))
        ]
        blocks_out = [jnp.where(why == 0, v, w) for v, w in zip(by_y[0], by_y[1])]
        blocks_out += [jnp.where(why == 0, w, v) for v, w in zip(by_y[0], by_y[1])]
        return jnp.concatenate(blocks_out, axis=0).T

    return jax.shard_map(
        local,
        mesh=grid,
        in_specs=(
            P(("rx", "rc", "cz", "cy"), None),
            P(("cz", "cy"), None),
            P(("rx", "rc"), ("cz", "cy")),
            P(("rx", "rc"), ("cz", "cy")),
            P(("rx", "rc"), ("cz", "cy"), None),
            P(("rx", "rc"), None, ("cz", "cy"), None),
        ),
        out_specs=P(("rx", "rc", "cz", "cy"), None),
        check_vma=False,
    )
```

```python
import jax
import jax.numpy as jnp
from jax import lax
from jax.experimental import pallas as pl
from jax.experimental.pallas import tpu as pltpu
from jax.sharding import Mesh, PartitionSpec as P

AXES = ("cz", "cy", "rx", "rc")


def solution(mesh):
    cols, rows = mesh.shape["col"], mesh.shape["row"]
    sizes = (cols // 2, 2, rows // 2, 2)
    grid = Mesh(mesh.devices.reshape(sizes), AXES)
    count_z, _, count_x, _ = sizes
    bf16 = jnp.bfloat16

    def place(z, y, x, c):
        return ((z * 2 + y) * sizes[2] + x) * 2 + c

    def send(value, target, only=None):
        pairs = []
        for z in range(sizes[0]):
            for y in range(2):
                for x in range(sizes[2]):
                    for c in range(2):
                        if only is None or only(z, y, x, c):
                            pairs.append((place(z, y, x, c), place(*target(z, y, x, c))))
        return lax.ppermute(value, AXES, pairs)

    def over_y(z, y, x, c):
        return z, 1 - y, x, c

    def over_core(z, y, x, c):
        return z, y, x, 1 - c

    def over_both(z, y, x, c):
        return z, 1 - y, x, 1 - c

    def picked(flag, why, vectors, own, own_y, other, other_y, first):
        count = len(vectors)
        part, depth = vectors[0].shape
        each = own.shape[1]

        def kernel(flags, *refs):
            vector_refs = refs[:count]
            own_ref, own_y_ref, other_ref, other_y_ref, out_ref, held, sems = refs[count:]

            def copies(near, far):
                return [
                    pltpu.make_async_copy(
                        ref.at[first + index], held.at[2 * index + side], sems.at[2 * index + side]
                    )
                    for index in range(count)
                    for side, ref in enumerate((near, far))
                ]

            @pl.when(flags[0] == 0)
            def _():
                for copy in copies(own_ref, own_y_ref):
                    copy.start()

            @pl.when(flags[0] != 0)
            def _():
                for copy in copies(other_ref, other_y_ref):
                    copy.start()

            results = [0.0, 0.0]
            for slot, copy in enumerate(copies(own_ref, own_y_ref)):
                copy.wait()
                results[slot % 2] += lax.dot_general(
                    held[slot], vector_refs[slot // 2][...], (((1,), (1,)), ((), ())),
                    preferred_element_type=jnp.float32,
                )
            results = [value.T for value in results]
            straight = flags[1] == 0
            out_ref[:, :each] = jnp.where(straight, results[0], results[1])
            out_ref[:, each:] = jnp.where(straight, results[1], results[0])

        whole = pl.BlockSpec(memory_space=pltpu.VMEM)
        far = pl.BlockSpec(memory_space=pl.ANY)
        return pl.pallas_call(
            kernel,
            in_specs=[pl.BlockSpec(memory_space=pltpu.SMEM)] + [whole] * count + [far] * 4,
            out_specs=whole,
            scratch_shapes=[
                pltpu.VMEM((2 * count, each, depth), bf16),
                pltpu.SemaphoreType.DMA((2 * count,)),
            ],
            out_shape=jax.ShapeDtypeStruct((part, 2 * each), jnp.float32),
            cost_estimate=pl.CostEstimate(
                flops=4 * count * part * depth * each,
                bytes_accessed=4 * count * each * depth,
                transcendentals=0,
            ),
            compiler_params=pltpu.CompilerParams(vmem_limit_bytes=(4 + 4 * count) * 1024 * 1024),
        )(jnp.stack([flag, why]).astype(jnp.int32), *vectors, own, own_y, other, other_y)

    def prior_parts(zed, why, right_side, prior_solution, factor_codes, block_scale):
        each, width = right_side.shape
        panel, depth = factor_codes.shape
        blocks = block_scale.shape[1]
        deep = depth // blocks
        chunk = 2 * each

        def kernel(place_ref, scale_ref, right_ref, prior_ref, codes_ref, out_ref, scaled, total):
            step = pl.program_id(0)

            @pl.when(step == 0)
            def _():
                for b in range(blocks):
                    part = prior_ref[b * deep : (b + 1) * deep, :].astype(jnp.float32)
                    scaled[b * deep : (b + 1) * deep, :] = (part * scale_ref[0, b]).astype(bf16)

            total[...] = -jnp.dot(
                codes_ref[...], scaled[...], preferred_element_type=jnp.float32
            )

            @pl.when(step == place_ref[0])
            def _():
                rows = pl.ds(pl.multiple_of(place_ref[1] * each, each), each)
                total[rows, :] += right_ref[...]

            out_ref[0] = total[...].T.astype(bf16)

        return pl.pallas_call(
            kernel,
            grid_spec=pltpu.PrefetchScalarGridSpec(
                num_scalar_prefetch=1,
                grid=(panel // chunk,),
                in_specs=[
                    pl.BlockSpec(memory_space=pltpu.SMEM),
                    pl.BlockSpec((each, width), lambda i, p: (0, 0)),
                    pl.BlockSpec((depth, width), lambda i, p: (0, 0)),
                    pl.BlockSpec((chunk, depth), lambda i, p: (i, 0)),
                ],
                out_specs=pl.BlockSpec((1, width, chunk), lambda i, p: (i, 0, 0)),
                scratch_shapes=[
                    pltpu.VMEM((depth, width), bf16),
                    pltpu.VMEM((chunk, width), jnp.float32),
                ],
            ),
            out_shape=jax.ShapeDtypeStruct((panel // chunk, width, chunk), bf16),
            cost_estimate=pl.CostEstimate(
                flops=2 * panel * depth * width,
                bytes_accessed=2 * panel * depth + 4 * panel * width,
                transcendentals=0,
            ),
            compiler_params=pltpu.CompilerParams(vmem_limit_bytes=60 * 1024 * 1024),
        )(jnp.stack([zed, why]).astype(jnp.int32), block_scale, right_side, prior_solution, factor_codes)

    def local(right_side, prior_solution, factor_codes, block_scale, diag_inverse, inner_factor):
        each, width = right_side.shape
        part = width // 4
        zed, why = lax.axis_index("cz"), lax.axis_index("cy")
        ex, core = lax.axis_index("rx"), lax.axis_index("rc")
        chunk = 2 * each
        panel = factor_codes.shape[0]

        def gather(piece, swap=None):
            def flip(x):
                return x if swap is None else swap[::-1][swap.index(x)] if x in swap else x

            if count_z > 4:
                if swap is not None:
                    piece = send(piece, lambda z, y, x, c: (z, y, flip(x), c))
                return jnp.moveaxis(lax.all_gather(piece, "cz", axis=0), 0, 1).reshape(part, panel)
            whole = jnp.zeros((part, panel), piece.dtype)
            got = [(zed, piece)] if swap is None else []
            for step in range(1 if swap is None else 0, count_z):

                def along(z, y, x, c):
                    return (z + step) % count_z, y, flip(x), c

                moved = send(piece, along)
                got.append((lax.rem(zed + count_z - step, count_z), moved))
            for source, value in got:
                whole = lax.dynamic_update_slice(whole, value, (0, source * chunk))
            return whole

        def apply(pieces, vector):
            mine, beside = [
                lax.dot_general(
                    vector, piece, (((1,), (1,)), ((), ())), preferred_element_type=jnp.float32
                )
                for piece in pieces
            ]
            first = jnp.where(why == 0, mine, beside)
            second = jnp.where(why == 0, beside, mine)
            return jnp.concatenate([first, second], axis=1)

        def again(value):
            return jnp.where(ex < count_x, value, -value)

        def pick(even, odd):
            return lax.optimization_barrier(jnp.where(core == 0, even, odd))

        before = 2 * (count_x - 1)
        inverse = diag_inverse[0]
        turns = range(count_x)

        def inverse_at(turn):
            if turn == 0:
                return lambda z, y, x, c: x == 0 or c == 0
            return lambda z, y, x, c: x == turn and c == 1

        def odd_at(turn):
            return lambda z, y, x, c: x == turn and c == 1

        past = inner_factor[0, :before]
        past_y = send(past, over_y, lambda z, y, x, c: x > 0)
        pair = lax.dynamic_index_in_dim(inner_factor[0], 2 * ex, 0, keepdims=False)
        inverse_c = send(inverse, over_core)
        pair_c = send(pair, over_core)
        past_c = send(past, over_core)
        past_yc = send(past_y, over_core)
        pair_y, pair_yc, inverse_y, inverse_yc = {}, {}, {}, {}
        for turn in turns:
            inverse_y[turn] = send(inverse, over_y, inverse_at(turn))
            inverse_yc[turn] = send(inverse_y[turn], over_core)
            pair_y[turn] = send(pair, over_y, odd_at(turn))
            pair_yc[turn] = send(pair_y[turn], over_core)
        near_even, near_odd = pick(inverse, inverse_c), pick(inverse_c, inverse)
        near_link = pick(pair_c, pair)
        inv_even = (near_even, pick(inverse_y[0], inverse_yc[0]))
        link, inv_odd = {}, {}
        for turn in turns:
            inv_odd[turn] = (near_odd, pick(inverse_yc[turn], inverse_y[turn]))
            link[turn] = (near_link, pick(pair_yc[turn], pair_y[turn]))

        parts = prior_parts(zed, why, right_side, prior_solution, factor_codes, block_scale)
        parts = parts.reshape(count_z * 4, part, chunk)
        came = lax.all_to_all(parts, ("cz", "cy", "rc"), 0, 0)
        came = came.reshape(count_z * 2, 2, part, chunk)
        rhs_even = came[:, 0].astype(jnp.float32).sum(0)
        came, rhs_even = lax.optimization_barrier((came, rhs_even))
        rhs_odd = came[:, 1].astype(jnp.float32).sum(0)

        kept = (None, None)
        for turn in turns:
            vector = gather(rhs_even.astype(bf16))
            even = apply(inv_even, vector)
            even_all = gather(even.astype(bf16))
            current = rhs_odd - apply(link[turn], even_all)
            vector = gather(current.astype(bf16))
            odd = apply(inv_odd[turn], vector)
            kept = [
                new if turn == 0 else jnp.where(ex == turn, new, old)
                for new, old in zip((even, odd), kept)
            ]
            for later in range(turn + 1, count_x):

                def exchange(z, y, x, c):
                    return z, y, later if x == turn else turn if x == later else x, c

                seen_even = send(again(even_all), exchange)
                seen_odd = gather(odd.astype(bf16), [turn, later])
                here = ex == later
                add = picked(core, why, [seen_even], past, past_y, past_c, past_yc, 2 * turn)
                near = pick(past[2 * turn + 1], past_c[2 * turn + 1])
                far = pick(past_y[2 * turn + 1], past_yc[2 * turn + 1])
                add = add + apply((near, far), seen_odd)
                rhs_even = rhs_even - jnp.where(here, add, 0.0)
                seen = [seen_even, again(seen_odd)]
                add = picked(
                    1 - core, why, seen, past, past_y, past_c, past_yc, 2 * turn
                )
                rhs_odd = rhs_odd - jnp.where(here, add, 0.0)

        near = [jnp.where(why == 0, v[:, :each], v[:, each:]) for v in kept]
        far = [jnp.where(why == 0, v[:, each:], v[:, :each]) for v in kept]
        mine = jnp.where(core == 0, near[0], near[1])
        from_y = send(jnp.where(core == 0, far[0], far[1]).astype(bf16), over_y)
        from_yc = send(jnp.where(core == 0, far[1], far[0]).astype(bf16), over_both)
        from_c = send(jnp.where(core == 0, near[1], near[0]), over_core)
        from_y, from_yc = from_y.astype(jnp.float32), from_yc.astype(jnp.float32)
        by_y = [
            (jnp.where(core == 0, v, w), jnp.where(core == 0, w, v))
            for v, w in ((mine, from_c), (from_y, from_yc))
        ]
        blocks_out = [jnp.where(why == 0, v, w) for v, w in zip(by_y[0], by_y[1])]
        blocks_out += [jnp.where(why == 0, w, v) for v, w in zip(by_y[0], by_y[1])]
        return jnp.concatenate(blocks_out, axis=0).T

    return jax.shard_map(
        local,
        mesh=grid,
        in_specs=(
            P(("rx", "rc", "cz", "cy"), None),
            P(("cz", "cy"), None),
            P(("rx", "rc"), ("cz", "cy")),
            P(("rx", "rc"), ("cz", "cy")),
            P(("rx", "rc"), ("cz", "cy"), None),
            P(("rx", "rc"), None, ("cz", "cy"), None),
        ),
        out_specs=P(("rx", "rc", "cz", "cy"), None),
        check_vma=False,
    )
```

```python
import jax
import jax.numpy as jnp
from jax import lax
from jax.experimental import pallas as pl
from jax.experimental.pallas import tpu as pltpu
from jax.sharding import Mesh, PartitionSpec as P

AXES = ("cz", "cy", "rx", "rc")


def solution(mesh):
    cols, rows = mesh.shape["col"], mesh.shape["row"]
    sizes = (cols // 2, 2, rows // 2, 2)
    grid = Mesh(mesh.devices.reshape(sizes), AXES)
    count_z, _, count_x, _ = sizes
    bf16 = jnp.bfloat16

    def place(z, y, x, c):
        return ((z * 2 + y) * sizes[2] + x) * 2 + c

    def send(value, target, only=None):
        pairs = []
        for z in range(sizes[0]):
            for y in range(2):
                for x in range(sizes[2]):
                    for c in range(2):
                        if only is None or only(z, y, x, c):
                            pairs.append((place(z, y, x, c), place(*target(z, y, x, c))))
        return lax.ppermute(value, AXES, pairs)

    def over_y(z, y, x, c):
        return z, 1 - y, x, c

    def over_core(z, y, x, c):
        return z, y, x, 1 - c

    def over_both(z, y, x, c):
        return z, 1 - y, x, 1 - c

    def picked(flag, why, vectors, own, own_y, other, other_y, first):
        count = len(vectors)
        part, depth = vectors[0].shape
        each = own.shape[1]

        def kernel(flags, *refs):
            vector_refs = refs[:count]
            own_ref, own_y_ref, other_ref, other_y_ref, out_ref, held, sems = refs[count:]

            def copies(near, far):
                return [
                    pltpu.make_async_copy(
                        ref.at[first + index], held.at[2 * index + side], sems.at[2 * index + side]
                    )
                    for index in range(count)
                    for side, ref in enumerate((near, far))
                ]

            @pl.when(flags[0] == 0)
            def _():
                for copy in copies(own_ref, own_y_ref):
                    copy.start()

            @pl.when(flags[0] != 0)
            def _():
                for copy in copies(other_ref, other_y_ref):
                    copy.start()

            results = [0.0, 0.0]
            for slot, copy in enumerate(copies(own_ref, own_y_ref)):
                copy.wait()
                results[slot % 2] += lax.dot_general(
                    held[slot], vector_refs[slot // 2][...], (((1,), (1,)), ((), ())),
                    preferred_element_type=jnp.float32,
                )
            results = [value.T for value in results]
            straight = flags[1] == 0
            out_ref[:, :each] = jnp.where(straight, results[0], results[1])
            out_ref[:, each:] = jnp.where(straight, results[1], results[0])

        whole = pl.BlockSpec(memory_space=pltpu.VMEM)
        far = pl.BlockSpec(memory_space=pl.ANY)
        return pl.pallas_call(
            kernel,
            in_specs=[pl.BlockSpec(memory_space=pltpu.SMEM)] + [whole] * count + [far] * 4,
            out_specs=whole,
            scratch_shapes=[
                pltpu.VMEM((2 * count, each, depth), bf16),
                pltpu.SemaphoreType.DMA((2 * count,)),
            ],
            out_shape=jax.ShapeDtypeStruct((part, 2 * each), jnp.float32),
            cost_estimate=pl.CostEstimate(
                flops=4 * count * part * depth * each,
                bytes_accessed=4 * count * each * depth,
                transcendentals=0,
            ),
            compiler_params=pltpu.CompilerParams(vmem_limit_bytes=(4 + 4 * count) * 1024 * 1024),
        )(jnp.stack([flag, why]).astype(jnp.int32), *vectors, own, own_y, other, other_y)

    def prior_parts(right_side, prior_solution, factor_codes, block_scale):
        each, width = right_side.shape
        panel, depth = factor_codes.shape
        blocks = block_scale.shape[1]
        deep = depth // blocks
        chunk = 2 * each

        def kernel(scale_ref, right_ref, prior_ref, codes_ref, out_ref, scaled, total):
            step = pl.program_id(0)
            zed, why = lax.axis_index("cz"), lax.axis_index("cy")

            @pl.when(step == 0)
            def _():
                for b in range(blocks):
                    part = prior_ref[b * deep : (b + 1) * deep, :].astype(jnp.float32)
                    scaled[b * deep : (b + 1) * deep, :] = (part * scale_ref[0, b]).astype(bf16)

            total[...] = -jnp.dot(
                codes_ref[...], scaled[...], preferred_element_type=jnp.float32
            )

            @pl.when(step == zed)
            def _():
                rows = pl.ds(pl.multiple_of(why * each, each), each)
                total[rows, :] += right_ref[...]

            out_ref[0] = total[...].T.astype(bf16)

        return pl.pallas_call(
            kernel,
            grid_spec=pltpu.PrefetchScalarGridSpec(
                num_scalar_prefetch=0,
                grid=(panel // chunk,),
                in_specs=[
                    pl.BlockSpec(memory_space=pltpu.SMEM),
                    pl.BlockSpec((each, width), lambda i: (0, 0)),
                    pl.BlockSpec((depth, width), lambda i: (0, 0)),
                    pl.BlockSpec((chunk, depth), lambda i: (i, 0)),
                ],
                out_specs=pl.BlockSpec((1, width, chunk), lambda i: (i, 0, 0)),
                scratch_shapes=[
                    pltpu.VMEM((depth, width), bf16),
                    pltpu.VMEM((chunk, width), jnp.float32),
                ],
            ),
            out_shape=jax.ShapeDtypeStruct((panel // chunk, width, chunk), bf16),
            cost_estimate=pl.CostEstimate(
                flops=2 * panel * depth * width,
                bytes_accessed=2 * panel * depth + 4 * panel * width,
                transcendentals=0,
            ),
            compiler_params=pltpu.CompilerParams(vmem_limit_bytes=60 * 1024 * 1024),
        )(block_scale, right_side, prior_solution, factor_codes)

    def local(right_side, prior_solution, factor_codes, block_scale, diag_inverse, inner_factor):
        each, width = right_side.shape
        part = width // 4
        zed, why = lax.axis_index("cz"), lax.axis_index("cy")
        ex, core = lax.axis_index("rx"), lax.axis_index("rc")
        chunk = 2 * each
        panel = factor_codes.shape[0]

        def gather(piece, swap=None):
            def flip(x):
                return x if swap is None else swap[::-1][swap.index(x)] if x in swap else x

            if count_z > 4:
                if swap is not None:
                    piece = send(piece, lambda z, y, x, c: (z, y, flip(x), c))
                return jnp.moveaxis(lax.all_gather(piece, "cz", axis=0), 0, 1).reshape(part, panel)
            whole = jnp.zeros((part, panel), piece.dtype)
            got = [(zed, piece)] if swap is None else []
            for step in range(1 if swap is None else 0, count_z):

                def along(z, y, x, c):
                    return (z + step) % count_z, y, flip(x), c

                moved = send(piece, along)
                got.append((lax.rem(zed + count_z - step, count_z), moved))
            for source, value in got:
                whole = lax.dynamic_update_slice(whole, value, (0, source * chunk))
            return whole

        def apply(pieces, vector):
            mine, beside = [
                lax.dot_general(
                    vector, piece, (((1,), (1,)), ((), ())), preferred_element_type=jnp.float32
                )
                for piece in pieces
            ]
            first = jnp.where(why == 0, mine, beside)
            second = jnp.where(why == 0, beside, mine)
            return jnp.concatenate([first, second], axis=1)

        def again(value):
            return jnp.where(ex < count_x, value, -value)

        def pick(even, odd):
            return lax.optimization_barrier(jnp.where(core == 0, even, odd))

        before = 2 * (count_x - 1)
        inverse = diag_inverse[0]
        turns = range(count_x)

        def inverse_at(turn):
            if turn == 0:
                return lambda z, y, x, c: x == 0 or c == 0
            return lambda z, y, x, c: x == turn and c == 1

        def odd_at(turn):
            return lambda z, y, x, c: x == turn and c == 1

        past = inner_factor[0, :before]
        past_y = send(past, over_y, lambda z, y, x, c: x > 0)
        pair = lax.dynamic_index_in_dim(inner_factor[0], 2 * ex, 0, keepdims=False)
        inverse_c = send(inverse, over_core)
        pair_c = send(pair, over_core)
        past_c = send(past, over_core)
        past_yc = send(past_y, over_core)
        pair_y, pair_yc, inverse_y, inverse_yc = {}, {}, {}, {}
        for turn in turns:
            inverse_y[turn] = send(inverse, over_y, inverse_at(turn))
            inverse_yc[turn] = send(inverse_y[turn], over_core)
            pair_y[turn] = send(pair, over_y, odd_at(turn))
            pair_yc[turn] = send(pair_y[turn], over_core)
        near_even, near_odd = pick(inverse, inverse_c), pick(inverse_c, inverse)
        near_link = pick(pair_c, pair)
        inv_even = (near_even, pick(inverse_y[0], inverse_yc[0]))
        link, inv_odd = {}, {}
        for turn in turns:
            inv_odd[turn] = (near_odd, pick(inverse_yc[turn], inverse_y[turn]))
            link[turn] = (near_link, pick(pair_yc[turn], pair_y[turn]))

        parts = prior_parts(right_side, prior_solution, factor_codes, block_scale)
        parts = parts.reshape(count_z * 4, part, chunk)
        came = lax.all_to_all(parts, ("cz", "cy", "rc"), 0, 0)
        came = came.reshape(count_z * 2, 2, part, chunk)
        rhs_even = came[:, 0].astype(jnp.float32).sum(0)
        came, rhs_even = lax.optimization_barrier((came, rhs_even))
        rhs_odd = came[:, 1].astype(jnp.float32).sum(0)

        kept = (None, None)
        for turn in turns:
            vector = gather(rhs_even.astype(bf16))
            even = apply(inv_even, vector)
            even_all = gather(even.astype(bf16))
            current = rhs_odd - apply(link[turn], even_all)
            vector = gather(current.astype(bf16))
            odd = apply(inv_odd[turn], vector)
            kept = [
                new if turn == 0 else jnp.where(ex == turn, new, old)
                for new, old in zip((even, odd), kept)
            ]
            for later in range(turn + 1, count_x):

                def exchange(z, y, x, c):
                    return z, y, later if x == turn else turn if x == later else x, c

                seen_even = send(again(even_all), exchange)
                seen_odd = gather(odd.astype(bf16), [turn, later])
                here = ex == later
                add = picked(core, why, [seen_even], past, past_y, past_c, past_yc, 2 * turn)
                near = pick(past[2 * turn + 1], past_c[2 * turn + 1])
                far = pick(past_y[2 * turn + 1], past_yc[2 * turn + 1])
                add = add + apply((near, far), seen_odd)
                rhs_even = rhs_even - jnp.where(here, add, 0.0)
                seen = [seen_even, again(seen_odd)]
                add = picked(
                    1 - core, why, seen, past, past_y, past_c, past_yc, 2 * turn
                )
                rhs_odd = rhs_odd - jnp.where(here, add, 0.0)

        near = [jnp.where(why == 0, v[:, :each], v[:, each:]) for v in kept]
        far = [jnp.where(why == 0, v[:, each:], v[:, :each]) for v in kept]
        mine = jnp.where(core == 0, near[0], near[1])
        from_y = send(jnp.where(core == 0, far[0], far[1]).astype(bf16), over_y)
        from_yc = send(jnp.where(core == 0, far[1], far[0]).astype(bf16), over_both)
        from_c = send(jnp.where(core == 0, near[1], near[0]), over_core)
        from_y, from_yc = from_y.astype(jnp.float32), from_yc.astype(jnp.float32)
        by_y = [
            (jnp.where(core == 0, v, w), jnp.where(core == 0, w, v))
            for v, w in ((mine, from_c), (from_y, from_yc))
        ]
        blocks_out = [jnp.where(why == 0, v, w) for v, w in zip(by_y[0], by_y[1])]
        blocks_out += [jnp.where(why == 0, w, v) for v, w in zip(by_y[0], by_y[1])]
        return jnp.concatenate(blocks_out, axis=0).T

    return jax.shard_map(
        local,
        mesh=grid,
        in_specs=(
            P(("rx", "rc", "cz", "cy"), None),
            P(("cz", "cy"), None),
            P(("rx", "rc"), ("cz", "cy")),
            P(("rx", "rc"), ("cz", "cy")),
            P(("rx", "rc"), ("cz", "cy"), None),
            P(("rx", "rc"), None, ("cz", "cy"), None),
        ),
        out_specs=P(("rx", "rc", "cz", "cy"), None),
        check_vma=False,
    )
```
